1024 devices in a mesh: fsdp: 64 (over y, x_hi, core), dp: 16 (over z, x_lo).
Axes of the slice: x: 8 (x_hi: 4, x_lo: 2; x = x_hi * 2 + x_lo), y: 8, z: 8, core: 2. Of those that a mesh axis runs over, the one named last changes fastest.
Arguments:
- inputs: bfloat16 [262144, 2560], P(('fsdp', 'dp')), may hold values from -24 to 24
- value_cotangent: bfloat16 [262144, 512], P(('fsdp', 'dp')), may hold values from -0.03125 to 0.03125
- master: float32 [2560, 4, 128], P('fsdp', None, 'dp'), may hold values from -0.125 to 0.125
- first_moment: float32 [2560, 4, 128], P('fsdp', None, 'dp'), may hold values from -6 to 6
- second_moment: float32 [2560, 4, 128], P('fsdp', None, 'dp'), may hold values from 0.25 to 4
Outputs:
- moment_one_new: float32 [2560, 4, 128], P('fsdp', None, 'dp')
- moment_two_new: float32 [2560, 4, 128], P('fsdp', None, 'dp')
- master_new: float32 [2560, 4, 128], P('fsdp', None, 'dp')
- head_blocks: bfloat16 [64, 2560, 128], P('fsdp', None, 'dp')
The draws below stay inside these ranges and needn't reach their ends.
All inputs are finite; a program needn't handle non-finite values.
Results may differ from the reference program's by a relative error of at most 0.0018.
Values may be sent and summed in bfloat16 or wider, within the bound.
No kernel may reach another device: no remote copies, remote signals or barrier semaphores. Data moves between devices by JAX's collectives and lax.ppermute only.
A program may use at most 32 MiB of HBM per device.

```python
import math
import jax
import jax.numpy as jnp
from jax import lax

D_IN = 2560
KVH = 4
HEAD = 128
STEP = 8
TOK_DEV = 256
VW = 512
TOKENS_ALL = 262144
N_FSDP = 64
N_DP = 16


def strengthened(entries, rng, source, target, parts, factor):
    def block_of(axis_at):
        return (jnp.arange(entries.shape[axis_at]) // (entries.shape[axis_at] // parts)).reshape((-1,) + (1,) * (entries.ndim - 1 - axis_at))

    first = jax.random.permutation(rng, parts)[block_of(target)]
    far = (block_of(target) + parts // 2) % parts
    return jnp.where((block_of(source) == first) | (block_of(source) == far), factor * entries, entries)


def block_levels(stream_key, shape, cuts, smallest, largest):
    gain = 1.0
    for axis_at, blocks in cuts:
        heights = jax.random.uniform(jax.random.fold_in(jax.random.fold_in(stream_key, 6), axis_at), (blocks,), jnp.float32, smallest / len(cuts), largest / len(cuts))
        gain = gain * jnp.repeat(jnp.exp(heights), shape[axis_at] // blocks).reshape((-1,) + (1,) * (len(shape) - 1 - axis_at))
    return gain


def bell_draw(rng, extent, scale, limit, split=(), dtype=jnp.bfloat16):
    array = scale * jax.random.normal(rng, extent, jnp.float32)
    if split:
        array = array * block_levels(rng, extent, split, -0.22, 0.18)
    return jnp.clip(array, -limit, limit).astype(dtype)


def gaussian_with(key, shape, scale, limit, split, heavy, held_as=jnp.bfloat16):
    entries = scale * jax.random.normal(key, shape, jnp.float32)
    if split:
        entries = entries * block_levels(key, shape, split, -0.22, 0.18)
    return jnp.clip(strengthened(entries, jax.random.fold_in(key, 3), *heavy), -limit, limit).astype(held_as)


def setup_inputs(seed: int = 0) -> dict:
    splits = jax.random.split(jax.random.key(seed), 6)
    return {
        "inputs": gaussian_with(splits[0], (TOKENS_ALL, D_IN), 1.0, 24.0, ((0, 1024),), (0, 1, 512, 6.0)),
        "value_cotangent": bell_draw(splits[1], (TOKENS_ALL, VW), ((TOK_DEV * N_FSDP * N_DP) ** -0.5), 0.03125, ((0, 1024),)),
        "master": bell_draw(splits[2], (D_IN, KVH, HEAD), D_IN ** -0.5, 0.125, ((0, 64), (2, 16)), jnp.float32),
        "first_moment": bell_draw(splits[3], (D_IN, KVH, HEAD), 1.0, 6.0, ((0, 64), (2, 16)), jnp.float32),
        "second_moment": jnp.clip(jnp.exp(math.log(4.0) - 2.7725887 * jax.random.uniform(splits[4], (D_IN, KVH, HEAD), jnp.float32) ** block_levels(splits[4], (D_IN, KVH, HEAD), ((0, 64), (2, 16)), -0.2, 0.2)), 0.25, 4.0),
    }


beta_first = 0.9
beta_second = 0.95
learn_rate = 0.001
weight_decay = 0.1
epsilon = 1e-08

def reference(inputs, value_cotangent, master, first_moment, second_moment):
    gradient = lax.dot_general(inputs, value_cotangent, (((0,), (0,)), ((), ())), preferred_element_type=jnp.float32)
    gradient = gradient.reshape(D_IN, KVH, HEAD)
    moment_one_new = beta_first * first_moment + (1.0 - beta_first) * gradient
    moment_two_new = beta_second * second_moment + (1.0 - beta_second) * gradient * gradient
    correct_one = 1.0 - beta_first ** STEP
    correct_two = 1.0 - beta_second ** STEP
    update = moment_one_new / correct_one / (jnp.sqrt(moment_two_new / correct_two) + epsilon) + weight_decay * master
    master_new = master - learn_rate * update
    narrow_weight = master_new.astype(jnp.bfloat16)
    head_order = (jnp.arange(N_FSDP) % KVH).astype(jnp.int32)
    picked = jnp.take(narrow_weight, head_order, axis=1)
    head_blocks = jnp.transpose(picked, (1, 0, 2))
    return (moment_one_new, moment_two_new, master_new, head_blocks)
```

```python
import jax
import jax.numpy as jnp
from jax import lax
from jax.sharding import PartitionSpec as P

KVH = 4
HEAD = 128
STEP = 8


beta_first = 0.9
beta_second = 0.95
learn_rate = 0.001
weight_decay = 0.1
epsilon = 1e-08


def in_blocks(x, dim, devices):
    before, after = (x.shape[:dim], x.shape[dim + 1 :])
    return jnp.moveaxis(x.reshape(*before, devices, -1, *after), dim, 0)


def summed_on_arrival(x, axis, dim):
    devices = lax.axis_size(axis)
    tiles = lax.all_to_all(in_blocks(x, dim, devices), axis, 0, 0, tiled=True)
    return jnp.sum(tiles.astype(jnp.float32), axis=0)


def adam_update(gradient, moment_one, moment_two, weights):
    moment_one_new = beta_first * moment_one + (1.0 - beta_first) * gradient
    moment_two_new = beta_second * moment_two + (1.0 - beta_second) * gradient * gradient
    correct_one = 1.0 - beta_first**STEP
    correct_two = 1.0 - beta_second**STEP
    update = (
        moment_one_new / correct_one / (jnp.sqrt(moment_two_new / correct_two) + epsilon)
        + weight_decay * weights
    )
    return (moment_one_new, moment_two_new, weights - learn_rate * update)


def shards(inputs, value_cotangent, master, first_moment, second_moment):
    slice_width = master.shape[2]
    term = lax.dot_general(
        inputs, value_cotangent, (((0,), (0,)), ((), ())), preferred_element_type=jnp.float32
    )
    term = term.astype(jnp.bfloat16).reshape(-1, KVH, HEAD)
    column_part = summed_on_arrival(term, "dp", 2)
    grad_share = summed_on_arrival(column_part.astype(jnp.bfloat16), "fsdp", 0)
    moment_one_new, moment_two_new, master_new = adam_update(
        grad_share, first_moment, second_moment, master
    )
    narrow_weight = master_new.astype(jnp.bfloat16)
    by_head = jnp.transpose(narrow_weight, (1, 0, 2))
    outgoing = jnp.tile(by_head, (lax.axis_size("fsdp") // KVH, 1, 1))
    arrived = lax.all_to_all(outgoing, "fsdp", split_axis=0, concat_axis=0, tiled=True)
    tp_block = arrived.reshape(1, -1, slice_width)
    return (moment_one_new, moment_two_new, master_new, tp_block)


def solution(mesh):
    placed = (
        P(("fsdp", "dp"), None),
        P(("fsdp", "dp"), None),
        P("fsdp", None, "dp"),
        P("fsdp", None, "dp"),
        P("fsdp", None, "dp"),
    )
    return jax.shard_map(
        shards,
        mesh=mesh,
        in_specs=placed,
        out_specs=(
            P("fsdp", None, "dp"),
            P("fsdp", None, "dp"),
            P("fsdp", None, "dp"),
            P("fsdp", None, "dp"),
        ),
        check_vma=False,
    )
```

```python
import math

import jax
import jax.numpy as jnp
from jax import lax
from jax.experimental import pallas as pl
from jax.experimental.pallas import tpu as pltpu
from jax.sharding import Mesh
from jax.sharding import PartitionSpec as P

KVH = 4
HEAD = 128
STEP = 8
LANES = 128

beta_first = 0.9
beta_second = 0.95
learn_rate = 0.001
weight_decay = 0.1
epsilon = 1e-08

VMEM = pl.BlockSpec(memory_space=pltpu.VMEM)
SMEM = pl.BlockSpec(memory_space=pltpu.SMEM)


def one_hot(test):
    return jnp.where(test, 1.0, 0.0)


def column_order(z_hi, z_lo, x_lo):
    width = KVH * HEAD
    share = HEAD // (z_hi * z_lo * x_lo)
    old = lax.broadcasted_iota(jnp.int32, (width, width), 0)
    new = lax.broadcasted_iota(jnp.int32, (width, width), 1)
    j = new % share
    head = new // share % KVH
    zh = new // (share * KVH) % z_hi
    xl = new // (share * KVH * z_hi) % x_lo
    zl = new // (share * KVH * z_hi * x_lo)
    source = head * HEAD + ((zh * z_lo + zl) * x_lo + xl) * share + j
    return one_hot(old == source).astype(jnp.bfloat16)


def partial_kernel(sizes, rows, which, core_ref, x_ref, cot_ref, out_ref, acc):
    z_hi, z_lo, x_lo = sizes
    order = column_order(z_hi, z_lo, x_lo)
    cot = jnp.dot(cot_ref[...], order, preferred_element_type=jnp.float32).astype(jnp.bfloat16)
    parity = core_ref[0] if which == "keep" else 1 - core_ref[0]
    d_in = x_ref.shape[1]
    chunk = 640
    pairs = chunk // (2 * rows)
    for c in range(d_in // chunk):
        acc[...] = lax.dot_general(
            x_ref[:, c * chunk : (c + 1) * chunk],
            cot,
            (((0,), (0,)), ((), ())),
            preferred_element_type=jnp.float32,
        )
        for k in range(pairs):
            start = pl.multiple_of((2 * k + parity) * rows, 8)
            block = acc[pl.ds(start, rows), :]
            at = (c * pairs + k) * rows
            for b in range(z_lo * x_lo):
                out_ref[b, at : at + rows, :] = block[:, b * LANES : (b + 1) * LANES].astype(out_ref.dtype)


def partials(which, sizes, rows, core, x, cot):
    d_in = x.shape[1]
    blocks = sizes[1] * sizes[2]
    dtype = jnp.float32 if which == "keep" else jnp.bfloat16
    return pl.pallas_call(
        lambda *refs: partial_kernel(sizes, rows, which, *refs),
        out_shape=jax.ShapeDtypeStruct((blocks, d_in // 2, LANES), dtype),
        in_specs=[SMEM, VMEM, VMEM],
        out_specs=VMEM,
        scratch_shapes=[pltpu.VMEM((640, KVH * HEAD), jnp.float32)],
        cost_estimate=pl.CostEstimate(flops=2 * x.shape[0] * d_in * KVH * HEAD, bytes_accessed=3 << 20, transcendentals=0),
        name="partial_" + which,
    )(core, x, cot)


def regroup_kernel(z_hi, parts_ref, out_ref, acc):
    total = parts_ref[0].astype(jnp.float32)
    for k in range(1, parts_ref.shape[0]):
        total = total + parts_ref[k].astype(jnp.float32)
    acc[...] = total
    n = acc.shape[0] // z_hi
    width = LANES // z_hi
    lane = lax.broadcasted_iota(jnp.int32, (n, LANES), 1) // width
    quarters = [acc[pl.ds(q, n, stride=z_hi), :] for q in range(z_hi)]
    for zh in range(z_hi):
        out = jnp.zeros((n, LANES), jnp.float32)
        for q in range(z_hi):
            shift = (q - zh) * width % LANES
            moved = quarters[q] if shift == 0 else pltpu.roll(quarters[q], shift, 1)
            out = jnp.where(lane == q, moved, out)
        out_ref[zh] = out.astype(out_ref.dtype)


def regroup(parts, z_hi):
    rows = parts.shape[1]
    return pl.pallas_call(
        lambda *refs: regroup_kernel(z_hi, *refs),
        out_shape=jax.ShapeDtypeStruct((z_hi, rows // z_hi, LANES), jnp.bfloat16),
        in_specs=[VMEM],
        out_specs=VMEM,
        scratch_shapes=[pltpu.VMEM((rows, LANES), jnp.float32)],
        name="regroup",
    )(parts)


def adam_update(gradient, moment_one, moment_two, weights):
    moment_one_new = beta_first * moment_one + (1.0 - beta_first) * gradient
    moment_two_new = beta_second * moment_two + (1.0 - beta_second) * gradient * gradient
    correct_one = 1.0 - beta_first**STEP
    correct_two = 1.0 - beta_second**STEP
    update = (
        moment_one_new / correct_one / (jnp.sqrt(moment_two_new / correct_two) + epsilon)
        + weight_decay * weights
    )
    return (moment_one_new, moment_two_new, weights - learn_rate * update)


def shards(inputs, value_cotangent, master, first_moment, second_moment):
    fsdp = tuple(a for a in ("y", "xh", "c"))
    sizes = tuple(lax.axis_size(a) for a in ("zh", "zl", "xl"))
    rows, _, slice_width = master.shape
    core = lax.axis_index("c").astype(jnp.int32).reshape(1)
    outgoing = partials("send", sizes, rows, core, inputs, value_cotangent)
    arrived = lax.ppermute(outgoing, "c", [(0, 1), (1, 0)])
    kept = partials("keep", sizes, rows, core, inputs, value_cotangent)
    chip_sum = (kept + arrived.astype(jnp.float32)).astype(jnp.bfloat16)
    parts = lax.all_to_all(chip_sum, ("zl", "xl"), 0, 0, tiled=True)
    blocks = regroup(parts, sizes[0])
    peers = sizes[0] * lax.axis_size("y") * lax.axis_size("xh")
    terms = lax.all_to_all(blocks.reshape(peers, 2, -1), ("zh", "y", "xh"), 0, 0, tiled=True)
    gradient = jnp.sum(terms.astype(jnp.float32), axis=0).reshape(rows, KVH, slice_width)
    moment_one_new, moment_two_new, master_new = adam_update(
        gradient, first_moment, second_moment, master
    )
    by_head = jnp.transpose(master_new.astype(jnp.bfloat16), (1, 0, 2))
    devices = math.prod(lax.axis_size(a) for a in fsdp)
    outgoing = jnp.tile(by_head, (devices // KVH, 1, 1))
    arrived = lax.all_to_all(outgoing, fsdp, 0, 0, tiled=True)
    return (moment_one_new, moment_two_new, master_new, arrived.reshape(1, -1, slice_width))


def solution(mesh):
    grid = mesh.devices.reshape(8, 4, 2, 4, 2, 2)
    fine = Mesh(grid, ("y", "xh", "c", "zh", "zl", "xl"))
    fsdp, dp = ("y", "xh", "c"), ("zh", "zl", "xl")
    tokens = P(fsdp + dp, None)
    owned = P(fsdp, None, dp)
    return jax.shard_map(
        shards,
        mesh=fine,
        in_specs=(tokens, tokens, owned, owned, owned),
        out_specs=(owned, owned, owned, owned),
        check_vma=False,
    )
```

```python
import math

import jax
import jax.numpy as jnp
from jax import lax
from jax.experimental import pallas as pl
from jax.experimental.pallas import tpu as pltpu
from jax.sharding import Mesh
from jax.sharding import PartitionSpec as P

KVH = 4
HEAD = 128
STEP = 8
LANES = 128

beta_first = 0.9
beta_second = 0.95
learn_rate = 0.001
weight_decay = 0.1
epsilon = 1e-08

VMEM = pl.BlockSpec(memory_space=pltpu.VMEM)
SMEM = pl.BlockSpec(memory_space=pltpu.SMEM)


def one_hot(test):
    return jnp.where(test, 1.0, 0.0)


def column_order(z_hi, z_lo, x_lo):
    width = KVH * HEAD
    share = HEAD // (z_hi * z_lo * x_lo)
    old = lax.broadcasted_iota(jnp.int32, (width, width), 0)
    new = lax.broadcasted_iota(jnp.int32, (width, width), 1)
    j = new % share
    head = new // share % KVH
    zh = new // (share * KVH) % z_hi
    xl = new // (share * KVH * z_hi) % x_lo
    zl = new // (share * KVH * z_hi * x_lo)
    source = head * HEAD + ((zh * z_lo + zl) * x_lo + xl) * share + j
    return one_hot(old == source).astype(jnp.bfloat16)


def partial_kernel(sizes, rows, which, core_ref, x_ref, cot_ref, out_ref, acc):
    z_hi, z_lo, x_lo = sizes
    order = column_order(z_hi, z_lo, x_lo)
    cot = jnp.dot(cot_ref[...], order, preferred_element_type=jnp.float32).astype(jnp.bfloat16)
    parity = core_ref[0] if which == "keep" else 1 - core_ref[0]
    chunk = acc.shape[1]
    pairs = chunk // (2 * rows)
    for c in range(x_ref.shape[1] // chunk):
        slot = c % acc.shape[0]
        acc[slot] = lax.dot_general(
            x_ref[:, c * chunk : (c + 1) * chunk],
            cot,
            (((0,), (0,)), ((), ())),
            preferred_element_type=jnp.float32,
        )
        for k in range(pairs):
            start = pl.multiple_of((2 * k + parity) * rows, 8)
            block = acc[slot, pl.ds(start, rows), :]
            at = (c * pairs + k) * rows
            for b in range(z_lo * x_lo):
                out_ref[b, at : at + rows, :] = block[:, b * LANES : (b + 1) * LANES].astype(out_ref.dtype)


def partials(which, sizes, rows, core, x, cot):
    tokens, d_in = x.shape
    blocks = sizes[1] * sizes[2]
    dtype = jnp.float32 if which == "keep" else jnp.bfloat16
    return pl.pallas_call(
        lambda *refs: partial_kernel(sizes, rows, which, *refs),
        out_shape=jax.ShapeDtypeStruct((blocks, d_in // 2, LANES), dtype),
        in_specs=[SMEM, VMEM, VMEM],
        out_specs=VMEM,
        scratch_shapes=[pltpu.VMEM((2, 640, KVH * HEAD), jnp.float32)],
        cost_estimate=pl.CostEstimate(flops=2 * tokens * d_in * KVH * HEAD, bytes_accessed=3 << 20, transcendentals=0),
        compiler_params=pltpu.CompilerParams(vmem_limit_bytes=16 << 20),
        name="partial_" + which,
    )(core, x, cot)


def regroup_kernel(z_hi, parts_ref, out_ref, acc):
    total = parts_ref[0].astype(jnp.float32)
    for k in range(1, parts_ref.shape[0]):
        total = total + parts_ref[k].astype(jnp.float32)
    acc[...] = total
    n = acc.shape[0] // z_hi
    width = LANES // z_hi
    lane = lax.broadcasted_iota(jnp.int32, (n, LANES), 1) // width
    quarters = [acc[pl.ds(q, n, stride=z_hi), :] for q in range(z_hi)]
    for zh in range(z_hi):
        out = jnp.zeros((n, LANES), jnp.float32)
        for q in range(z_hi):
            shift = (q - zh) * width % LANES
            moved = quarters[q] if shift == 0 else pltpu.roll(quarters[q], shift, 1)
            out = jnp.where(lane == q, moved, out)
        out_ref[zh * n : (zh + 1) * n, :] = out.astype(out_ref.dtype)


def regroup(parts, z_hi):
    rows = parts.shape[1]
    return pl.pallas_call(
        lambda *refs: regroup_kernel(z_hi, *refs),
        out_shape=jax.ShapeDtypeStruct((rows, LANES), jnp.bfloat16),
        in_specs=[VMEM],
        out_specs=VMEM,
        scratch_shapes=[pltpu.VMEM((rows, LANES), jnp.float32)],
        compiler_params=pltpu.CompilerParams(vmem_limit_bytes=16 << 20),
        name="regroup",
    )(parts)


def adam_update(gradient, moment_one, moment_two, weights):
    moment_one_new = beta_first * moment_one + (1.0 - beta_first) * gradient
    moment_two_new = beta_second * moment_two + (1.0 - beta_second) * gradient * gradient
    correct_one = 1.0 - beta_first**STEP
    correct_two = 1.0 - beta_second**STEP
    update = (
        moment_one_new / correct_one / (jnp.sqrt(moment_two_new / correct_two) + epsilon)
        + weight_decay * weights
    )
    return (moment_one_new, moment_two_new, weights - learn_rate * update)


def shards(inputs, value_cotangent, master, first_moment, second_moment):
    fsdp = tuple(a for a in ("y", "xh", "c"))
    sizes = tuple(lax.axis_size(a) for a in ("zh", "zl", "xl"))
    rows, _, slice_width = master.shape
    core = lax.axis_index("c").astype(jnp.int32).reshape(1)
    outgoing = partials("send", sizes, rows, core, inputs, value_cotangent)
    arrived = lax.ppermute(outgoing, "c", [(0, 1), (1, 0)])
    kept = partials("keep", sizes, rows, core, inputs, value_cotangent)
    chip_sum = (kept + arrived.astype(jnp.float32)).astype(jnp.bfloat16)
    parts = lax.all_to_all(chip_sum, ("zl", "xl"), 0, 0, tiled=True)
    blocks = regroup(parts, sizes[0])
    peers = sizes[0] * lax.axis_size("y") * lax.axis_size("xh")
    terms = lax.all_to_all(blocks.reshape(-1, 2, LANES), ("zh", "y", "xh"), 0, 0, tiled=True)
    terms = terms.reshape(peers, -1, 2, LANES).astype(jnp.float32)
    gradient = jnp.sum(terms, axis=0).reshape(rows, KVH, slice_width)
    moment_one_new, moment_two_new, master_new = adam_update(
        gradient, first_moment, second_moment, master
    )
    by_head = jnp.transpose(master_new.astype(jnp.bfloat16), (1, 0, 2))
    devices = math.prod(lax.axis_size(a) for a in fsdp)
    outgoing = jnp.tile(by_head, (devices // KVH, 1, 1))
    arrived = lax.all_to_all(outgoing, fsdp, 0, 0, tiled=True)
    return (moment_one_new, moment_two_new, master_new, arrived.reshape(1, -1, slice_width))


def solution(mesh):
    grid = mesh.devices.reshape(8, 4, 2, 4, 2, 2)
    fine = Mesh(grid, ("y", "xh", "c", "zh", "zl", "xl"))
    fsdp, dp = ("y", "xh", "c"), ("zh", "zl", "xl")
    tokens = P(fsdp + dp, None)
    owned = P(fsdp, None, dp)
    return jax.shard_map(
        shards,
        mesh=fine,
        in_specs=(tokens, tokens, owned, owned, owned),
        out_specs=(owned, owned, owned, owned),
        check_vma=False,
    )
```

```python
import math

import jax
import jax.numpy as jnp
from jax import lax
from jax.experimental import pallas as pl
from jax.experimental.pallas import tpu as pltpu
from jax.sharding import Mesh
from jax.sharding import PartitionSpec as P

KVH = 4
HEAD = 128
STEP = 8
LANES = 128

beta_first = 0.9
beta_second = 0.95
learn_rate = 0.001
weight_decay = 0.1
epsilon = 1e-08

VMEM = pl.BlockSpec(memory_space=pltpu.VMEM)
SMEM = pl.BlockSpec(memory_space=pltpu.SMEM)


def one_hot(test):
    return jnp.where(test, 1.0, 0.0)


def column_order(z_hi, z_lo, x_lo):
    width = KVH * HEAD
    share = HEAD // (z_hi * z_lo * x_lo)
    old = lax.broadcasted_iota(jnp.int32, (width, width), 0)
    new = lax.broadcasted_iota(jnp.int32, (width, width), 1)
    j = new % share
    head = new // share % KVH
    zh = new // (share * KVH) % z_hi
    xl = new // (share * KVH * z_hi) % x_lo
    zl = new // (share * KVH * z_hi * x_lo)
    source = head * HEAD + ((zh * z_lo + zl) * x_lo + xl) * share + j
    return one_hot(old == source).astype(jnp.bfloat16)


def partial_kernel(sizes, rows, which, core_ref, x_ref, cot_ref, out_ref, acc, held, held_cot, sems):
    z_hi, z_lo, x_lo = sizes
    chunks, _, chunk = held.shape
    copies = [pltpu.make_async_copy(cot_ref, held_cot, sems.at[chunks])]
    copies += [
        pltpu.make_async_copy(x_ref.at[:, pl.ds(c * chunk, chunk)], held.at[c], sems.at[c]) for c in range(chunks)
    ]
    for copy in copies:
        copy.start()
    order = column_order(z_hi, z_lo, x_lo)
    copies[0].wait()
    cot = jnp.dot(held_cot[...], order, preferred_element_type=jnp.float32).astype(jnp.bfloat16)
    parity = core_ref[0] if which == "keep" else 1 - core_ref[0]
    pairs = chunk // (2 * rows)
    for c in range(chunks):
        copies[c + 1].wait()
        slot = c % acc.shape[0]
        acc[slot] = lax.dot_general(
            held[c], cot, (((0,), (0,)), ((), ())), preferred_element_type=jnp.float32
        )
        for k in range(pairs):
            start = pl.multiple_of((2 * k + parity) * rows, 8)
            block = acc[slot, pl.ds(start, rows), :]
            at = (c * pairs + k) * rows
            for b in range(z_lo * x_lo):
                out_ref[b, at : at + rows, :] = block[:, b * LANES : (b + 1) * LANES].astype(out_ref.dtype)


def partials(which, sizes, rows, core, x, cot):
    tokens, d_in = x.shape
    blocks = sizes[1] * sizes[2]
    dtype = jnp.float32 if which == "keep" else jnp.bfloat16
    chunk = 640
    anywhere = pl.BlockSpec(memory_space=pl.ANY)
    return pl.pallas_call(
        lambda *refs: partial_kernel(sizes, rows, which, *refs),
        out_shape=jax.ShapeDtypeStruct((blocks, d_in // 2, LANES), dtype),
        in_specs=[SMEM, anywhere, anywhere],
        out_specs=VMEM,
        scratch_shapes=[
            pltpu.VMEM((2, chunk, KVH * HEAD), jnp.float32),
            pltpu.VMEM((d_in // chunk, tokens, chunk), jnp.bfloat16),
            pltpu.VMEM(cot.shape, jnp.bfloat16),
            pltpu.SemaphoreType.DMA((d_in // chunk + 1,)),
        ],
        cost_estimate=pl.CostEstimate(flops=2 * tokens * d_in * KVH * HEAD, bytes_accessed=3 << 20, transcendentals=0),
        compiler_params=pltpu.CompilerParams(vmem_limit_bytes=16 << 20),
        name="partial_" + which,
    )(core, *(pltpu.with_memory_space_constraint(a, pltpu.HBM) for a in (x, cot)))


def regroup_kernel(z_hi, parts_ref, out_ref, acc):
    total = parts_ref[0].astype(jnp.float32)
    for k in range(1, parts_ref.shape[0]):
        total = total + parts_ref[k].astype(jnp.float32)
    acc[...] = total
    n = acc.shape[0] // z_hi
    width = LANES // z_hi
    lane = lax.broadcasted_iota(jnp.int32, (n, LANES), 1) // width
    quarters = [acc[pl.ds(q, n, stride=z_hi), :] for q in range(z_hi)]
    for zh in range(z_hi):
        out = jnp.zeros((n, LANES), jnp.float32)
        for q in range(z_hi):
            shift = (q - zh) * width % LANES
            moved = quarters[q] if shift == 0 else pltpu.roll(quarters[q], shift, 1)
            out = jnp.where(lane == q, moved, out)
        out_ref[zh * n : (zh + 1) * n, :] = out.astype(out_ref.dtype)


def regroup(parts, z_hi):
    rows = parts.shape[1]
    return pl.pallas_call(
        lambda *refs: regroup_kernel(z_hi, *refs),
        out_shape=jax.ShapeDtypeStruct((rows, LANES), jnp.bfloat16),
        in_specs=[VMEM],
        out_specs=VMEM,
        scratch_shapes=[pltpu.VMEM((rows, LANES), jnp.float32)],
        compiler_params=pltpu.CompilerParams(vmem_limit_bytes=16 << 20),
        name="regroup",
    )(parts)


def adam_update(gradient, moment_one, moment_two, weights):
    moment_one_new = beta_first * moment_one + (1.0 - beta_first) * gradient
    moment_two_new = beta_second * moment_two + (1.0 - beta_second) * gradient * gradient
    correct_one = 1.0 - beta_first**STEP
    correct_two = 1.0 - beta_second**STEP
    update = (
        moment_one_new / correct_one / (jnp.sqrt(moment_two_new / correct_two) + epsilon)
        + weight_decay * weights
    )
    return (moment_one_new, moment_two_new, weights - learn_rate * update)


def shards(inputs, value_cotangent, master, first_moment, second_moment):
    fsdp = tuple(a for a in ("y", "xh", "c"))
    sizes = tuple(lax.axis_size(a) for a in ("zh", "zl", "xl"))
    rows, _, slice_width = master.shape
    core = lax.axis_index("c").astype(jnp.int32).reshape(1)
    outgoing = partials("send", sizes, rows, core, inputs, value_cotangent)
    arrived = lax.ppermute(outgoing, "c", [(0, 1), (1, 0)])
    kept = partials("keep", sizes, rows, core, inputs, value_cotangent)
    chip_sum = (kept + arrived.astype(jnp.float32)).astype(jnp.bfloat16)
    parts = lax.all_to_all(chip_sum, ("zl", "xl"), 0, 0, tiled=True)
    blocks = regroup(parts, sizes[0])
    peers = sizes[0] * lax.axis_size("y") * lax.axis_size("xh")
    terms = lax.all_to_all(blocks.reshape(-1, 2, LANES), ("zh", "y", "xh"), 0, 0, tiled=True)
    terms = terms.reshape(peers, -1, 2, LANES).astype(jnp.float32)
    gradient = jnp.sum(terms, axis=0).reshape(rows, KVH, slice_width)
    moment_one_new, moment_two_new, master_new = adam_update(
        gradient, first_moment, second_moment, master
    )
    by_head = jnp.transpose(master_new.astype(jnp.bfloat16), (1, 0, 2))
    devices = math.prod(lax.axis_size(a) for a in fsdp)
    outgoing = jnp.tile(by_head, (devices // KVH, 1, 1))
    arrived = lax.all_to_all(outgoing, fsdp, 0, 0, tiled=True)
    return (moment_one_new, moment_two_new, master_new, arrived.reshape(1, -1, slice_width))


def solution(mesh):
    grid = mesh.devices.reshape(8, 4, 2, 4, 2, 2)
    fine = Mesh(grid, ("y", "xh", "c", "zh", "zl", "xl"))
    fsdp, dp = ("y", "xh", "c"), ("zh", "zl", "xl")
    tokens = P(fsdp + dp, None)
    owned = P(fsdp, None, dp)
    return jax.shard_map(
        shards,
        mesh=fine,
        in_specs=(tokens, tokens, owned, owned, owned),
        out_specs=(owned, owned, owned, owned),
        check_vma=False,
    )
```

```python
import math

import jax
import jax.numpy as jnp
from jax import lax
from jax.experimental import pallas as pl
from jax.experimental.pallas import tpu as pltpu
from jax.sharding import Mesh
from jax.sharding import PartitionSpec as P

KVH = 4
HEAD = 128
STEP = 8
LANES = 128

beta_first = 0.9
beta_second = 0.95
learn_rate = 0.001
weight_decay = 0.1
epsilon = 1e-08

VMEM = pl.BlockSpec(memory_space=pltpu.VMEM)
SMEM = pl.BlockSpec(memory_space=pltpu.SMEM)


def one_hot(test):
    return jnp.where(test, 1.0, 0.0)


def column_order(z_hi, z_lo, x_lo):
    width = KVH * HEAD
    share = HEAD // (z_hi * z_lo * x_lo)
    old = lax.broadcasted_iota(jnp.int32, (width, width), 0)
    new = lax.broadcasted_iota(jnp.int32, (width, width), 1)
    j = new % share
    head = new // share % KVH
    zh = new // (share * KVH) % z_hi
    xl = new // (share * KVH * z_hi) % x_lo
    zl = new // (share * KVH * z_hi * x_lo)
    source = head * HEAD + ((zh * z_lo + zl) * x_lo + xl) * share + j
    return one_hot(old == source).astype(jnp.bfloat16)


def partial_kernel(sizes, rows, which, core_ref, x_ref, cot_ref, out_ref, acc, held, held_cot, sems):
    z_hi, z_lo, x_lo, y_lo, x_hi = sizes
    chunks, _, chunk = held.shape
    copies = [pltpu.make_async_copy(cot_ref, held_cot, sems.at[chunks])]
    copies += [
        pltpu.make_async_copy(x_ref.at[:, pl.ds(c * chunk, chunk)], held.at[c], sems.at[c]) for c in range(chunks)
    ]
    for copy in copies:
        copy.start()
    order = column_order(z_hi, z_lo, x_lo)
    copies[0].wait()
    cot = jnp.dot(held_cot[...], order, preferred_element_type=jnp.float32).astype(jnp.bfloat16)
    parity = core_ref[0] if which == "keep" else 1 - core_ref[0]
    pairs = chunk // (2 * rows)
    span = x_hi * rows
    for c in range(chunks):
        copies[c + 1].wait()
        slot = c % acc.shape[0]
        acc[slot] = lax.dot_general(
            held[c], cot, (((0,), (0,)), ((), ())), preferred_element_type=jnp.float32
        )
        for k in range(pairs):
            start = pl.multiple_of((2 * k + parity) * rows, 8)
            block = acc[slot, pl.ds(start, rows), :]
            y, x = divmod(c * pairs + k, x_hi)
            at = y // y_lo * span + x * rows
            for b in range(z_lo * x_lo):
                out_ref[y % y_lo * z_lo * x_lo + b, at : at + rows, :] = block[:, b * LANES : (b + 1) * LANES].astype(out_ref.dtype)


def partials(which, sizes, rows, core, x, cot):
    tokens, d_in = x.shape
    blocks = math.prod(sizes[1:4])
    dtype = jnp.float32 if which == "keep" else jnp.bfloat16
    chunk = 640
    anywhere = pl.BlockSpec(memory_space=pl.ANY)
    return pl.pallas_call(
        lambda *refs: partial_kernel(sizes, rows, which, *refs),
        out_shape=jax.ShapeDtypeStruct((blocks, 2 * d_in // blocks, LANES), dtype),
        in_specs=[SMEM, anywhere, anywhere],
        out_specs=VMEM,
        scratch_shapes=[
            pltpu.VMEM((2, chunk, KVH * HEAD), jnp.float32),
            pltpu.VMEM((d_in // chunk, tokens, chunk), jnp.bfloat16),
            pltpu.VMEM(cot.shape, jnp.bfloat16),
            pltpu.SemaphoreType.DMA((d_in // chunk + 1,)),
        ],
        cost_estimate=pl.CostEstimate(flops=2 * tokens * d_in * KVH * HEAD, bytes_accessed=3 << 20, transcendentals=0),
        compiler_params=pltpu.CompilerParams(vmem_limit_bytes=16 << 20),
        name="partial_" + which,
    )(core, *(pltpu.with_memory_space_constraint(a, pltpu.HBM) for a in (x, cot)))


def regroup_kernel(z_hi, parts_ref, out_ref, acc):
    total = parts_ref[0].astype(jnp.float32)
    for k in range(1, parts_ref.shape[0]):
        total = total + parts_ref[k].astype(jnp.float32)
    acc[...] = total
    n = acc.shape[0] // z_hi
    width = LANES // z_hi
    lane = lax.broadcasted_iota(jnp.int32, (n, LANES), 1) // width
    quarters = [acc[pl.ds(q, n, stride=z_hi), :] for q in range(z_hi)]
    for zh in range(z_hi):
        out = jnp.zeros((n, LANES), jnp.float32)
        for q in range(z_hi):
            shift = (q - zh) * width % LANES
            moved = quarters[q] if shift == 0 else pltpu.roll(quarters[q], shift, 1)
            out = jnp.where(lane == q, moved, out)
        out_ref[zh * n : (zh + 1) * n, :] = out.astype(out_ref.dtype)


def regroup(parts, z_hi):
    rows = parts.shape[1]
    return pl.pallas_call(
        lambda *refs: regroup_kernel(z_hi, *refs),
        out_shape=jax.ShapeDtypeStruct((rows, LANES), jnp.bfloat16),
        in_specs=[VMEM],
        out_specs=VMEM,
        scratch_shapes=[pltpu.VMEM((rows, LANES), jnp.float32)],
        compiler_params=pltpu.CompilerParams(vmem_limit_bytes=16 << 20),
        name="regroup",
    )(parts)


def adam_update(gradient, moment_one, moment_two, weights):
    moment_one_new = beta_first * moment_one + (1.0 - beta_first) * gradient
    moment_two_new = beta_second * moment_two + (1.0 - beta_second) * gradient * gradient
    correct_one = 1.0 - beta_first**STEP
    correct_two = 1.0 - beta_second**STEP
    update = (
        moment_one_new / correct_one / (jnp.sqrt(moment_two_new / correct_two) + epsilon)
        + weight_decay * weights
    )
    return (moment_one_new, moment_two_new, weights - learn_rate * update)


def shards(inputs, value_cotangent, master, first_moment, second_moment):
    fsdp = ("yh", "yl", "xh", "c")
    sizes = tuple(lax.axis_size(a) for a in ("zh", "zl", "xl", "yl", "xh"))
    rows, _, slice_width = master.shape
    core = lax.axis_index("c").astype(jnp.int32).reshape(1)
    outgoing = partials("send", sizes, rows, core, inputs, value_cotangent)
    arrived = lax.ppermute(outgoing, "c", [(0, 1), (1, 0)])
    kept = partials("keep", sizes, rows, core, inputs, value_cotangent)
    chip_sum = (kept + arrived.astype(jnp.float32)).astype(jnp.bfloat16)
    parts = lax.all_to_all(chip_sum, ("yl", "zl", "xl"), 0, 0, tiled=True)
    blocks = regroup(parts, sizes[0])
    peers = sizes[0] * lax.axis_size("yh") * lax.axis_size("xh")
    terms = lax.all_to_all(blocks.reshape(-1, 2, LANES), ("zh", "yh", "xh"), 0, 0, tiled=True)
    terms = terms.reshape(peers, -1, 2, LANES).astype(jnp.float32)
    gradient = jnp.sum(terms, axis=0).reshape(rows, KVH, slice_width)
    moment_one_new, moment_two_new, master_new = adam_update(
        gradient, first_moment, second_moment, master
    )
    by_head = jnp.transpose(master_new.astype(jnp.bfloat16), (1, 0, 2))
    devices = math.prod(lax.axis_size(a) for a in fsdp)
    outgoing = jnp.tile(by_head, (devices // KVH, 1, 1))
    arrived = lax.all_to_all(outgoing, fsdp, 0, 0, tiled=True)
    return (moment_one_new, moment_two_new, master_new, arrived.reshape(1, -1, slice_width))


def solution(mesh):
    grid = mesh.devices.reshape(4, 2, 4, 2, 4, 2, 2)
    fine = Mesh(grid, ("yh", "yl", "xh", "c", "zh", "zl", "xl"))
    fsdp, dp = ("yh", "yl", "xh", "c"), ("zh", "zl", "xl")
    tokens = P(fsdp + dp, None)
    owned = P(fsdp, None, dp)
    return jax.shard_map(
        shards,
        mesh=fine,
        in_specs=(tokens, tokens, owned, owned, owned),
        out_specs=(owned, owned, owned, owned),
        check_vma=False,
    )
```

```python
import itertools
import math

import jax
import jax.numpy as jnp
import numpy as np
from jax import lax
from jax.experimental import pallas as pl
from jax.experimental.pallas import tpu as pltpu
from jax.sharding import Mesh
from jax.sharding import PartitionSpec as P

KVH = 4
HEAD = 128
STEP = 8
LANES = 128
ALL_AXES = ("yh", "yl", "xh", "c", "zh", "zl", "xl")

beta_first = 0.9
beta_second = 0.95
learn_rate = 0.001
weight_decay = 0.1
epsilon = 1e-08

VMEM = pl.BlockSpec(memory_space=pltpu.VMEM)
SMEM = pl.BlockSpec(memory_space=pltpu.SMEM)


def one_hot(test):
    return jnp.where(test, 1.0, 0.0)


def column_order(z_hi, z_lo, x_lo):
    width = KVH * HEAD
    share = HEAD // (z_hi * z_lo * x_lo)
    old = lax.broadcasted_iota(jnp.int32, (width, width), 0)
    new = lax.broadcasted_iota(jnp.int32, (width, width), 1)
    j = new % share
    head = new // share % KVH
    zh = new // (share * KVH) % z_hi
    xl = new // (share * KVH * z_hi) % x_lo
    zl = new // (share * KVH * z_hi * x_lo)
    source = head * HEAD + ((zh * z_lo + zl) * x_lo + xl) * share + j
    return one_hot(old == source).astype(jnp.bfloat16)


def partial_kernel(sizes, rows, which, core_ref, x_ref, cot_ref, out_ref, acc, held, held_cot, sems):
    z_hi, z_lo, x_lo, y_lo, x_hi = sizes
    chunks, _, chunk = held.shape
    copies = [pltpu.make_async_copy(cot_ref, held_cot, sems.at[chunks])]
    copies += [
        pltpu.make_async_copy(x_ref.at[:, pl.ds(c * chunk, chunk)], held.at[c], sems.at[c]) for c in range(chunks)
    ]
    for copy in copies:
        copy.start()
    order = column_order(z_hi, z_lo, x_lo)
    copies[0].wait()
    cot = jnp.dot(held_cot[...], order, preferred_element_type=jnp.float32).astype(jnp.bfloat16)
    parity = core_ref[0] if which == "keep" else 1 - core_ref[0]
    pairs = chunk // (2 * rows)
    span = x_hi * rows
    for c in range(chunks):
        copies[c + 1].wait()
        slot = c % acc.shape[0]
        acc[slot] = lax.dot_general(
            held[c], cot, (((0,), (0,)), ((), ())), preferred_element_type=jnp.float32
        )
        for k in range(pairs):
            start = pl.multiple_of((2 * k + parity) * rows, 8)
            block = acc[slot, pl.ds(start, rows), :]
            y, x = divmod(c * pairs + k, x_hi)
            at = y // y_lo * span + x * rows
            for b in range(z_lo * x_lo):
                out_ref[y % y_lo * z_lo * x_lo + b, at : at + rows, :] = block[:, b * LANES : (b + 1) * LANES].astype(out_ref.dtype)


def partials(which, sizes, rows, core, x, cot):
    tokens, d_in = x.shape
    blocks = math.prod(sizes[1:4])
    dtype = jnp.float32 if which == "keep" else jnp.bfloat16
    chunk = 640
    anywhere = pl.BlockSpec(memory_space=pl.ANY)
    return pl.pallas_call(
        lambda *refs: partial_kernel(sizes, rows, which, *refs),
        out_shape=jax.ShapeDtypeStruct((blocks, 2 * d_in // blocks, LANES), dtype),
        in_specs=[SMEM, anywhere, anywhere],
        out_specs=VMEM,
        scratch_shapes=[
            pltpu.VMEM((2, chunk, KVH * HEAD), jnp.float32),
            pltpu.VMEM((d_in // chunk, tokens, chunk), jnp.bfloat16),
            pltpu.VMEM(cot.shape, jnp.bfloat16),
            pltpu.SemaphoreType.DMA((d_in // chunk + 1,)),
        ],
        cost_estimate=pl.CostEstimate(flops=2 * tokens * d_in * KVH * HEAD, bytes_accessed=3 << 20, transcendentals=0),
        compiler_params=pltpu.CompilerParams(vmem_limit_bytes=16 << 20),
        name="partial_" + which,
    )(core, *(pltpu.with_memory_space_constraint(a, pltpu.HBM) for a in (x, cot)))


def regroup_kernel(z_hi, parts_ref, out_ref, acc):
    total = parts_ref[0].astype(jnp.float32)
    for k in range(1, parts_ref.shape[0]):
        total = total + parts_ref[k].astype(jnp.float32)
    acc[...] = total
    n = acc.shape[0] // z_hi
    width = LANES // z_hi
    lane = lax.broadcasted_iota(jnp.int32, (n, LANES), 1) // width
    quarters = [acc[pl.ds(q, n, stride=z_hi), :] for q in range(z_hi)]
    for zh in range(z_hi):
        out = jnp.zeros((n, LANES), jnp.float32)
        for q in range(z_hi):
            shift = (q - zh) * width % LANES
            moved = quarters[q] if shift == 0 else pltpu.roll(quarters[q], shift, 1)
            out = jnp.where(lane == q, moved, out)
        out_ref[zh * n : (zh + 1) * n, :] = out.astype(out_ref.dtype)


def regroup(parts, z_hi):
    rows = parts.shape[1]
    return pl.pallas_call(
        lambda *refs: regroup_kernel(z_hi, *refs),
        out_shape=jax.ShapeDtypeStruct((rows, LANES), jnp.bfloat16),
        in_specs=[VMEM],
        out_specs=VMEM,
        scratch_shapes=[pltpu.VMEM((rows, LANES), jnp.float32)],
        compiler_params=pltpu.CompilerParams(vmem_limit_bytes=16 << 20),
        name="regroup",
    )(parts)


def adam_update(gradient, moment_one, moment_two, weights):
    moment_one_new = beta_first * moment_one + (1.0 - beta_first) * gradient
    moment_two_new = beta_second * moment_two + (1.0 - beta_second) * gradient * gradient
    correct_one = 1.0 - beta_first**STEP
    correct_two = 1.0 - beta_second**STEP
    update = (
        moment_one_new / correct_one / (jnp.sqrt(moment_two_new / correct_two) + epsilon)
        + weight_decay * weights
    )
    return (moment_one_new, moment_two_new, weights - learn_rate * update)


def cubes(size):
    shape = tuple(size(a) for a in ALL_AXES)
    yh, yl, xh, cores, zh, zl, xl = shape
    groups = []
    for core, y0, z0, x0 in itertools.product(range(cores), range(yh), range(zh), range(xh)):
        group = []
        for py, pz, px in itertools.product(range(yl), range(zl), range(xl)):
            y = (y0 + (core and py == 0)) % yh
            z = (z0 + (core and pz == 0)) % zh
            x = (x0 + (core and px == 0)) % xh
            group.append(int(np.ravel_multi_index((y, py, x, core, z, pz, px), shape)))
        groups.append(group)
    return groups


def shards(inputs, value_cotangent, master, first_moment, second_moment):
    fsdp = ("yh", "yl", "xh", "c")
    sizes = tuple(lax.axis_size(a) for a in ("zh", "zl", "xl", "yl", "xh"))
    rows, _, slice_width = master.shape
    core = lax.axis_index("c").astype(jnp.int32).reshape(1)
    outgoing = partials("send", sizes, rows, core, inputs, value_cotangent)
    arrived = lax.ppermute(outgoing, "c", [(0, 1), (1, 0)])
    kept = partials("keep", sizes, rows, core, inputs, value_cotangent)
    chip_sum = (kept + arrived.astype(jnp.float32)).astype(jnp.bfloat16)
    parts = lax.all_to_all(
        chip_sum, ALL_AXES, 0, 0, axis_index_groups=cubes(lax.axis_size), tiled=True
    )
    blocks = regroup(parts, sizes[0])
    peers = sizes[0] * lax.axis_size("yh") * lax.axis_size("xh")
    terms = lax.all_to_all(blocks.reshape(-1, 2, LANES), ("zh", "yh", "xh"), 0, 0, tiled=True)
    terms = terms.reshape(peers, -1, 2, LANES).astype(jnp.float32)
    gradient = jnp.sum(terms, axis=0).reshape(rows, KVH, slice_width)
    moment_one_new, moment_two_new, master_new = adam_update(
        gradient, first_moment, second_moment, master
    )
    by_head = jnp.transpose(master_new.astype(jnp.bfloat16), (1, 0, 2))
    devices = math.prod(lax.axis_size(a) for a in fsdp)
    outgoing = jnp.tile(by_head, (devices // KVH, 1, 1))
    arrived = lax.all_to_all(outgoing, fsdp, 0, 0, tiled=True)
    return (moment_one_new, moment_two_new, master_new, arrived.reshape(1, -1, slice_width))


def solution(mesh):
    grid = mesh.devices.reshape(4, 2, 4, 2, 4, 2, 2)
    fine = Mesh(grid, ("yh", "yl", "xh", "c", "zh", "zl", "xl"))
    fsdp, dp = ("yh", "yl", "xh", "c"), ("zh", "zl", "xl")
    tokens = P(fsdp + dp, None)
    owned = P(fsdp, None, dp)
    return jax.shard_map(
        shards,
        mesh=fine,
        in_specs=(tokens, tokens, owned, owned, owned),
        out_specs=(owned, owned, owned, owned),
        check_vma=False,
    )
```

```python
import itertools
import math

import jax
import jax.numpy as jnp
import numpy as np
from jax import lax
from jax.experimental import pallas as pl
from jax.experimental.pallas import tpu as pltpu
from jax.sharding import Mesh
from jax.sharding import PartitionSpec as P

KVH = 4
HEAD = 128
STEP = 8
LANES = 128
ALL_AXES = ("yh", "yl", "xh", "c", "zh", "zl", "xl")

beta_first = 0.9
beta_second = 0.95
learn_rate = 0.001
weight_decay = 0.1
epsilon = 1e-08

VMEM = pl.BlockSpec(memory_space=pltpu.VMEM)
SMEM = pl.BlockSpec(memory_space=pltpu.SMEM)


def one_hot(test):
    return jnp.where(test, 1.0, 0.0)


def column_order(z_hi, z_lo, x_lo):
    width = KVH * HEAD
    share = HEAD // (z_hi * z_lo * x_lo)
    old = lax.broadcasted_iota(jnp.int32, (width, width), 0)
    new = lax.broadcasted_iota(jnp.int32, (width, width), 1)
    j = new % share
    head = new // share % KVH
    zh = new // (share * KVH) % z_hi
    xl = new // (share * KVH * z_hi) % x_lo
    zl = new // (share * KVH * z_hi * x_lo)
    source = head * HEAD + ((zh * z_lo + zl) * x_lo + xl) * share + j
    return one_hot(old == source).astype(jnp.bfloat16)


def partial_kernel(sizes, rows, which, core_ref, x_ref, cot_ref, out_ref, acc, held, held_cot, sems):
    z_hi, z_lo, x_lo, y_lo, x_hi = sizes
    chunks, _, chunk = held.shape
    copies = [pltpu.make_async_copy(cot_ref, held_cot, sems.at[chunks])]
    copies += [
        pltpu.make_async_copy(x_ref.at[:, pl.ds(c * chunk, chunk)], held.at[c], sems.at[c]) for c in range(chunks)
    ]
    for copy in copies:
        copy.start()
    order = column_order(z_hi, z_lo, x_lo)
    copies[0].wait()
    cot = jnp.dot(held_cot[...], order, preferred_element_type=jnp.float32).astype(jnp.bfloat16)
    parity = core_ref[0] if which == "keep" else 1 - core_ref[0]
    pairs = chunk // (2 * rows)
    span = x_hi * rows
    for c in range(chunks):
        copies[c + 1].wait()
        slot = c % acc.shape[0]
        acc[slot] = lax.dot_general(
            held[c], cot, (((0,), (0,)), ((), ())), preferred_element_type=jnp.float32
        )
        for k in range(pairs):
            start = pl.multiple_of((2 * k + parity) * rows, 8)
            block = acc[slot, pl.ds(start, rows), :]
            y, x = divmod(c * pairs + k, x_hi)
            at = y // y_lo * span + x * rows
            for b in range(z_lo * x_lo):
                out_ref[y % y_lo * z_lo * x_lo + b, at : at + rows, :] = block[:, b * LANES : (b + 1) * LANES].astype(out_ref.dtype)


def partials(which, sizes, rows, core, x, cot):
    tokens, d_in = x.shape
    blocks = math.prod(sizes[1:4])
    dtype = jnp.float32 if which == "keep" else jnp.bfloat16
    chunk = 1280
    anywhere = pl.BlockSpec(memory_space=pl.ANY)
    return pl.pallas_call(
        lambda *refs: partial_kernel(sizes, rows, which, *refs),
        out_shape=jax.ShapeDtypeStruct((blocks, 2 * d_in // blocks, LANES), dtype),
        in_specs=[SMEM, anywhere, anywhere],
        out_specs=VMEM,
        scratch_shapes=[
            pltpu.VMEM((2, chunk, KVH * HEAD), jnp.float32),
            pltpu.VMEM((d_in // chunk, tokens, chunk), jnp.bfloat16),
            pltpu.VMEM(cot.shape, jnp.bfloat16),
            pltpu.SemaphoreType.DMA((d_in // chunk + 1,)),
        ],
        cost_estimate=pl.CostEstimate(flops=2 * tokens * d_in * KVH * HEAD, bytes_accessed=3 << 20, transcendentals=0),
        compiler_params=pltpu.CompilerParams(vmem_limit_bytes=16 << 20),
        name="partial_" + which,
    )(core, *(pltpu.with_memory_space_constraint(a, pltpu.HBM) for a in (x, cot)))


def regroup_kernel(z_hi, parts_ref, out_ref, acc):
    total = parts_ref[0].astype(jnp.float32)
    for k in range(1, parts_ref.shape[0]):
        total = total + parts_ref[k].astype(jnp.float32)
    acc[...] = total
    n = acc.shape[0] // z_hi
    width = LANES // z_hi
    lane = lax.broadcasted_iota(jnp.int32, (n, LANES), 1) // width
    quarters = [acc[pl.ds(q, n, stride=z_hi), :] for q in range(z_hi)]
    for zh in range(z_hi):
        out = jnp.zeros((n, LANES), jnp.float32)
        for q in range(z_hi):
            shift = (q - zh) * width % LANES
            moved = quarters[q] if shift == 0 else pltpu.roll(quarters[q], shift, 1)
            out = jnp.where(lane == q, moved, out)
        out_ref[zh * n : (zh + 1) * n, :] = out.astype(out_ref.dtype)


def regroup(parts, z_hi):
    rows = parts.shape[1]
    return pl.pallas_call(
        lambda *refs: regroup_kernel(z_hi, *refs),
        out_shape=jax.ShapeDtypeStruct((rows, LANES), jnp.bfloat16),
        in_specs=[VMEM],
        out_specs=VMEM,
        scratch_shapes=[pltpu.VMEM((rows, LANES), jnp.float32)],
        compiler_params=pltpu.CompilerParams(vmem_limit_bytes=16 << 20),
        name="regroup",
    )(parts)


def adam_update(gradient, moment_one, moment_two, weights):
    moment_one_new = beta_first * moment_one + (1.0 - beta_first) * gradient
    moment_two_new = beta_second * moment_two + (1.0 - beta_second) * gradient * gradient
    correct_one = 1.0 - beta_first**STEP
    correct_two = 1.0 - beta_second**STEP
    update = (
        moment_one_new / correct_one / (jnp.sqrt(moment_two_new / correct_two) + epsilon)
        + weight_decay * weights
    )
    return (moment_one_new, moment_two_new, weights - learn_rate * update)


def cubes(size):
    shape = tuple(size(a) for a in ALL_AXES)
    yh, yl, xh, cores, zh, zl, xl = shape
    groups = []
    for core, y0, z0, x0 in itertools.product(range(cores), range(yh), range(zh), range(xh)):
        group = []
        for py, pz, px in itertools.product(range(yl), range(zl), range(xl)):
            y = (y0 + (core and py == 0)) % yh
            z = (z0 + (core and pz == 0)) % zh
            x = (x0 + (core and px == 0)) % xh
            group.append(int(np.ravel_multi_index((y, py, x, core, z, pz, px), shape)))
        groups.append(group)
    return groups


def shards(inputs, value_cotangent, master, first_moment, second_moment):
    fsdp = ("yh", "yl", "xh", "c")
    sizes = tuple(lax.axis_size(a) for a in ("zh", "zl", "xl", "yl", "xh"))
    rows, _, slice_width = master.shape
    core = lax.axis_index("c").astype(jnp.int32).reshape(1)
    outgoing = partials("send", sizes, rows, core, inputs, value_cotangent)
    arrived = lax.ppermute(outgoing, "c", [(0, 1), (1, 0)])
    kept = partials("keep", sizes, rows, core, inputs, value_cotangent)
    chip_sum = (kept + arrived.astype(jnp.float32)).astype(jnp.bfloat16)
    parts = lax.all_to_all(
        chip_sum, ALL_AXES, 0, 0, axis_index_groups=cubes(lax.axis_size), tiled=True
    )
    blocks = regroup(parts, sizes[0])
    peers = sizes[0] * lax.axis_size("yh") * lax.axis_size("xh")
    terms = lax.all_to_all(blocks.reshape(-1, 2, LANES), ("zh", "yh", "xh"), 0, 0, tiled=True)
    terms = terms.reshape(peers, -1, 2, LANES).astype(jnp.float32)
    gradient = jnp.sum(terms, axis=0).reshape(rows, KVH, slice_width)
    moment_one_new, moment_two_new, master_new = adam_update(
        gradient, first_moment, second_moment, master
    )
    by_head = jnp.transpose(master_new.astype(jnp.bfloat16), (1, 0, 2))
    devices = math.prod(lax.axis_size(a) for a in fsdp)
    outgoing = jnp.tile(by_head, (devices // KVH, 1, 1))
    arrived = lax.all_to_all(outgoing, fsdp, 0, 0, tiled=True)
    return (moment_one_new, moment_two_new, master_new, arrived.reshape(1, -1, slice_width))


def solution(mesh):
    grid = mesh.devices.reshape(4, 2, 4, 2, 4, 2, 2)
    fine = Mesh(grid, ("yh", "yl", "xh", "c", "zh", "zl", "xl"))
    fsdp, dp = ("yh", "yl", "xh", "c"), ("zh", "zl", "xl")
    tokens = P(fsdp + dp, None)
    owned = P(fsdp, None, dp)
    return jax.shard_map(
        shards,
        mesh=fine,
        in_specs=(tokens, tokens, owned, owned, owned),
        out_specs=(owned, owned, owned, owned),
        check_vma=False,
    )
```
